8 devices in a mesh: rep: 1 (over z), data: 2 (over y), model: 4 (over x, core).
Axes of the slice: x: 2, y: 2, z: 1, core: 2. Of those that a mesh axis runs over, the one named last changes fastest.
Arguments:
- x: bfloat16 [4, 2048, 2048], P(('rep', 'data'), 'model')
- lengths: int32 [4], P(('rep', 'data'))
- gamma: bfloat16 [2, 2048], P(None, 'data')
- w_in: bfloat16 [2, 2048, 34816], P(None, 'data', 'model')
- w_kv: bfloat16 [2, 2048, 512], P(None, 'data')
- w_out: bfloat16 [2, 18432, 2048], P(None, 'model', 'data')
Outputs:
- output: bfloat16 [4, 2048, 2048], P(('rep', 'data'), 'model')
All inputs are finite; a program needn't handle non-finite values.
Results may differ from the reference program's by a relative error of at most 0.0141291.
Values are sent between devices in bfloat16 or wider.
A program may use at most 1 GiB of HBM per device.

```python
import jax
import jax.numpy as jnp
from jax import lax

BATCH_SIZE = 4
SEQ_LEN = 2048
D_MODEL = 2048
N_HEADS = 8
HEAD_DIM = 256
D_FF = 16384
N_SHARDS = 4

EPSILON = 1e-6
LOCAL_HEADS = N_HEADS // N_SHARDS
FF_LOCAL = D_FF // N_SHARDS
ATTN_COLS = LOCAL_HEADS * HEAD_DIM
IN_LOCAL = ATTN_COLS + 2 * FF_LOCAL
OUT_LOCAL = ATTN_COLS + FF_LOCAL
QUERY_BLOCK = SEQ_LEN // N_SHARDS


def setup_inputs(seed: int = 0, part: int = 0) -> dict:
    part_key = jax.random.fold_in(jax.random.key(seed), part)
    key_x, key_len_a, key_len_b = jax.random.split(part_key, 3)
    key_gain, key_in, key_kv, key_out = jax.random.split(jax.random.key(seed + 1), 4)
    x = jax.random.normal(key_x, (BATCH_SIZE, SEQ_LEN, D_MODEL), jnp.float32).astype(jnp.bfloat16)
    len_min = SEQ_LEN // 8
    len_a = jax.random.randint(key_len_a, (BATCH_SIZE,), len_min, SEQ_LEN + 1, jnp.int32)
    len_b = jax.random.randint(key_len_b, (BATCH_SIZE,), len_min, SEQ_LEN + 1, jnp.int32)
    lengths = jnp.maximum(len_a, len_b).at[0].set(SEQ_LEN).at[BATCH_SIZE - 1].set(len_min)
    gamma = (1.0 + 0.3 * jax.random.normal(key_gain, (2, D_MODEL), jnp.float32)).astype(jnp.bfloat16)
    w_in = (jax.random.normal(key_in, (2, D_MODEL, N_SHARDS * IN_LOCAL), jnp.float32) * D_MODEL ** -0.5).astype(jnp.bfloat16)
    w_kv = (jax.random.normal(key_kv, (2, D_MODEL, 2 * HEAD_DIM), jnp.float32) * (2.0 * D_MODEL ** -0.5)).astype(jnp.bfloat16)
    w_out = (jax.random.normal(key_out, (2, N_SHARDS * OUT_LOCAL, D_MODEL), jnp.float32) * (N_SHARDS * OUT_LOCAL) ** -0.5).astype(jnp.bfloat16)
    return {"x": x, "lengths": lengths, "gamma": gamma, "w_in": w_in, "w_kv": w_kv, "w_out": w_out}


def rms_norm(x_in, gain):
    x_f32 = x_in.astype(jnp.float32)
    inv_rms = lax.rsqrt(jnp.mean(x_f32 * x_f32, axis=-1, keepdims=True) + EPSILON)
    return (x_f32 * inv_rms * gain.astype(jnp.float32)).astype(jnp.bfloat16)


def attend_one(q_seq, k_seq, v_seq, seq_len):
    key_pos = jnp.arange(SEQ_LEN)
    q_blocks = q_seq.reshape(N_SHARDS, QUERY_BLOCK, N_HEADS, HEAD_DIM)
    k_f32 = k_seq.astype(jnp.float32)
    v_f32 = v_seq.astype(jnp.float32)

    def one_block(block_in):
        q_blk, blk_idx = block_in
        scores = jnp.einsum("qhd,kd->hqk", q_blk.astype(jnp.float32), k_f32) * (HEAD_DIM ** -0.5)
        q_pos = blk_idx * QUERY_BLOCK + jnp.arange(QUERY_BLOCK)
        visible = (key_pos[None, :] <= q_pos[:, None]) & (key_pos[None, :] < seq_len)
        scores = jnp.where(visible[None], scores, -1e30)
        attn_probs = jax.nn.softmax(scores, axis=-1).astype(jnp.bfloat16)
        blk_out = jnp.einsum("hqk,kd->qhd", attn_probs.astype(jnp.float32), v_f32)
        return blk_out.astype(jnp.bfloat16)

    blocks_out = lax.map(one_block, (q_blocks, jnp.arange(N_SHARDS)))
    return blocks_out.reshape(SEQ_LEN, N_SHARDS, ATTN_COLS)


def layer_one(x_seq, seq_len, gain, w_in_l, w_kv_l, w_out_l):
    normed = rms_norm(x_seq, gain)
    projected = jnp.dot(normed, w_in_l, preferred_element_type=jnp.float32).astype(jnp.bfloat16)
    projected = projected.reshape(SEQ_LEN, N_SHARDS, IN_LOCAL)
    queries = projected[:, :, :ATTN_COLS].reshape(SEQ_LEN, N_HEADS, HEAD_DIM)
    gate = projected[:, :, ATTN_COLS:ATTN_COLS + FF_LOCAL].astype(jnp.float32)
    up_proj = projected[:, :, ATTN_COLS + FF_LOCAL:].astype(jnp.float32)
    key_value = jnp.dot(normed, w_kv_l, preferred_element_type=jnp.float32).astype(jnp.bfloat16)
    attn_out = attend_one(queries, key_value[:, :HEAD_DIM], key_value[:, HEAD_DIM:], seq_len)
    mlp_out = (jax.nn.silu(gate) * up_proj).astype(jnp.bfloat16)
    mixed = jnp.moveaxis(jnp.concatenate([attn_out, mlp_out], axis=-1), 1, 0)
    w_out_groups = w_out_l.reshape(N_SHARDS, OUT_LOCAL, D_MODEL)

    def add_group(z_acc, group_in):
        rows, weights = group_in
        part_z = jnp.dot(rows, weights, preferred_element_type=jnp.float32).astype(jnp.bfloat16)
        return z_acc + part_z.astype(jnp.float32), None

    z_sum, _ = lax.scan(add_group, jnp.zeros((SEQ_LEN, D_MODEL), jnp.float32), (mixed, w_out_groups))
    return (x_seq.astype(jnp.float32) + z_sum).astype(jnp.bfloat16)


def reference(x, lengths, gamma, w_in, w_kv, w_out):
    def one_layer(hidden, params):
        gain, w_in_l, w_kv_l, w_out_l = params
        new_hidden = lax.map(lambda seq_in: layer_one(seq_in[0], seq_in[1], gain, w_in_l, w_kv_l, w_out_l), (hidden, lengths))
        return new_hidden, None

    result, _ = lax.scan(one_layer, x, (gamma, w_in, w_kv, w_out))
    return result
```

```python
import functools

import jax
import jax.numpy as jnp
from jax import lax
from jax.experimental import pallas as pl
from jax.experimental.pallas import tpu as pltpu
from jax.sharding import PartitionSpec as P

EPSILON = 1e-6
VMEM_LIMIT = 60 * 1024 * 1024
BF16 = jnp.bfloat16
F32 = jnp.float32


def rms_norm(x_in, gain):
    x_f32 = x_in.astype(F32)
    inv_rms = lax.rsqrt(jnp.mean(x_f32 * x_f32, axis=-1, keepdims=True) + EPSILON)
    return (x_f32 * inv_rms * gain.astype(F32)).astype(BF16)


def gated_kernel(idx_ref, h_ref, g_own, u_own, g_oth, u_oth, out_ref):
    half = g_own.shape[0]
    h_a = h_ref[:, :half]
    h_b = h_ref[:, half:]
    gate = jnp.dot(h_a, g_own[...], preferred_element_type=F32) + jnp.dot(h_b, g_oth[...], preferred_element_type=F32)
    up = jnp.dot(h_a, u_own[...], preferred_element_type=F32) + jnp.dot(h_b, u_oth[...], preferred_element_type=F32)
    gate = gate.astype(BF16).astype(F32)
    up = up.astype(BF16).astype(F32)
    out_ref[...] = (gate * jax.nn.sigmoid(gate) * up).astype(BF16)


def gated(h, w_own, w_oth, layer, idx, g_col, u_col, width, tile_m=1024, tile_n=512):
    rows, d_model = h.shape
    half = d_model // 2
    n_tiles = width // tile_n
    g_blk, u_blk = g_col // tile_n, u_col // tile_n
    return pl.pallas_call(
        gated_kernel,
        grid_spec=pltpu.PrefetchScalarGridSpec(
            num_scalar_prefetch=1,
            grid=(n_tiles, rows // tile_m),
            in_specs=[
                pl.BlockSpec((tile_m, d_model), lambda n, m, s: (m, 0)),
                pl.BlockSpec((None, half, tile_n), lambda n, m, s: (layer, 0, g_blk + s[0] + n)),
                pl.BlockSpec((None, half, tile_n), lambda n, m, s: (layer, 0, u_blk + s[0] + n)),
                pl.BlockSpec((half, tile_n), lambda n, m, s: (0, n)),
                pl.BlockSpec((half, tile_n), lambda n, m, s: (0, n_tiles + n)),
            ],
            out_specs=pl.BlockSpec((tile_m, tile_n), lambda n, m, s: (m, n)),
        ),
        out_shape=jax.ShapeDtypeStruct((rows, width), BF16),
        compiler_params=pltpu.CompilerParams(vmem_limit_bytes=VMEM_LIMIT),
        cost_estimate=pl.CostEstimate(flops=4 * rows * d_model * width, bytes_accessed=2 * (rows * d_model * n_tiles + 2 * d_model * width + rows * width), transcendentals=rows * width),
        name="gated",
    )(idx, h, w_own, w_own, w_oth, w_oth)


def project_kernel(n_lhs, *refs):
    lhs, w_ref, out_ref = refs[:n_lhs], refs[n_lhs], refs[n_lhs + 1]
    row = 0
    acc = None
    for ref in lhs:
        part = jnp.dot(ref[...], w_ref[row:row + ref.shape[1], :], preferred_element_type=F32)
        acc = part if acc is None else acc + part
        row += ref.shape[1]
    out_ref[...] = acc.astype(BF16)


def project(lhs, weights, layer=None, tile_m=1024, tile_n=512):
    rows = lhs[0].shape[0]
    depth, cols = weights.shape[-2:]
    tile_n = min(tile_n, cols)
    if layer is None:
        w_spec = pl.BlockSpec((depth, tile_n), lambda n, m: (0, n))
    else:
        w_spec = pl.BlockSpec((None, depth, tile_n), lambda n, m: (layer, 0, n))
    return pl.pallas_call(
        functools.partial(project_kernel, len(lhs)),
        grid=(cols // tile_n, rows // tile_m),
        in_specs=[pl.BlockSpec((tile_m, a.shape[1]), lambda n, m: (m, 0)) for a in lhs] + [w_spec],
        out_specs=pl.BlockSpec((tile_m, tile_n), lambda n, m: (m, n)),
        out_shape=jax.ShapeDtypeStruct((rows, cols), BF16),
        compiler_params=pltpu.CompilerParams(vmem_limit_bytes=VMEM_LIMIT),
        cost_estimate=pl.CostEstimate(flops=2 * rows * depth * cols, bytes_accessed=2 * (rows * depth * (cols // tile_n) + depth * cols + rows * cols), transcendentals=0),
        name="project",
    )(*lhs, weights)


def attend_kernel(block, n_blocks, lens_ref, q_ref, k_ref, v_ref, out_ref):
    seq_len = lens_ref[pl.program_id(0)]
    which = pl.program_id(2)
    head_dim = q_ref.shape[1]
    for blk in range(n_blocks):
        @pl.when(which == blk)
        def _(blk=blk):
            keys = (blk + 1) * block
            scores = lax.dot_general(q_ref[...], k_ref[:keys, :], (((1,), (1,)), ((), ())), preferred_element_type=F32) * (head_dim ** -0.5)
            key_pos = lax.broadcasted_iota(jnp.int32, (block, keys), 1)
            q_pos = blk * block + lax.broadcasted_iota(jnp.int32, (block, keys), 0)
            scores = jnp.where((key_pos <= q_pos) & (key_pos < seq_len), scores, -1e30)
            top = jnp.max(scores, axis=-1, keepdims=True)
            weights = jnp.exp(scores - top)
            probs = (weights / jnp.sum(weights, axis=-1, keepdims=True)).astype(BF16)
            out_ref[...] = jnp.dot(probs, v_ref[:keys, :], preferred_element_type=F32).astype(BF16)


def attend(qkv, lens, n_heads, head_dim, block=512):
    n_seq, length, _ = qkv.shape
    n_blocks = length // block
    flops = 4 * n_seq * n_heads * length * length * head_dim * 5 // 8
    return pl.pallas_call(
        functools.partial(attend_kernel, block, n_blocks),
        grid_spec=pltpu.PrefetchScalarGridSpec(
            num_scalar_prefetch=1,
            grid=(n_seq, n_heads, n_blocks),
            in_specs=[
                pl.BlockSpec((None, block, head_dim), lambda c, i, b, s: (c, b, i)),
                pl.BlockSpec((None, length, head_dim), lambda c, i, b, s: (c, 0, n_heads)),
                pl.BlockSpec((None, length, head_dim), lambda c, i, b, s: (c, 0, n_heads + 1)),
            ],
            out_specs=pl.BlockSpec((None, block, head_dim), lambda c, i, b, s: (c, b, i)),
        ),
        out_shape=jax.ShapeDtypeStruct((n_seq, length, n_heads * head_dim), BF16),
        compiler_params=pltpu.CompilerParams(vmem_limit_bytes=VMEM_LIMIT),
        cost_estimate=pl.CostEstimate(flops=flops, bytes_accessed=4 * n_seq * n_heads * length * head_dim * 4, transcendentals=n_seq * n_heads * length * length),
        name="attend",
    )(lens, qkv, qkv, qkv)


def same_kernel(x_ref, out_ref):
    out_ref[...] = x_ref[...]


def same(x):
    return pl.pallas_call(same_kernel, out_shape=jax.ShapeDtypeStruct(x.shape, x.dtype), name="same")(x)


def solution(mesh):
    batch_axes = ("rep", "data")
    n_model = mesh.shape["model"]
    swap = [(0, 1), (1, 0)]

    def across(value):
        return lax.ppermute(value, "data", swap)

    def gather_seq(value):
        return lax.all_gather(value, "model", axis=1, tiled=True)

    def scatter_seq(value):
        return lax.psum_scatter(value, "model", scatter_dimension=1, tiled=True)

    def local_body(x_loc, lens_loc, gamma_loc, w_in_loc, w_kv_loc, w_out_loc):
        n_batch, seq_loc, d_model = x_loc.shape
        half = d_model // 2
        head_dim = w_kv_loc.shape[2] // 2
        out_local = w_out_loc.shape[1]
        ff = w_in_loc.shape[2] - out_local
        attn_cols = out_local - ff
        n_heads = attn_cols // head_dim
        seq = seq_loc * n_model
        rows = n_batch * seq
        mine = lax.axis_index("data")
        theirs = 1 - mine
        slot = lax.axis_index("model")

        def swap_halves(value):
            return jnp.concatenate([value[..., half:], value[..., :half]], axis=-1)

        def own_first(value):
            return jnp.where(mine == 0, value, swap_halves(value))

        def cols(layer, start, width):
            return lax.dynamic_slice(w_in_loc, (layer, 0, start), (1, half, width))[0]

        gamma = jnp.concatenate([gamma_loc, across(gamma_loc)], axis=-1)
        lens_all = jnp.concatenate([lens_loc, across(lens_loc)])
        part = half // n_model
        kv_part = across(lax.dynamic_slice(w_kv_loc, (0, slot * part, 0), (2, part, 2 * head_dim)))
        kv_oth = gather_seq(kv_part)
        w_kv = jnp.concatenate([w_kv_loc, kv_oth], axis=1)

        b_q, b_ff = attn_cols // 2, ff // 2
        b_chunk = 512
        hidden = own_first(x_loc)
        normed = rms_norm(hidden, gamma[0])
        q_oth = across(cols(0, theirs * b_q, b_q))
        normed_oth = across(swap_halves(normed))
        in_oth = []
        for c in range(b_ff // b_chunk):
            start = attn_cols + theirs * b_ff + c * b_chunk
            in_oth.append(across(jnp.concatenate([cols(0, start, b_chunk), cols(0, ff + start, b_chunk)], axis=1)))

        def out_rows(which):
            top = lax.dynamic_slice(w_out_loc, (0, which * b_q, 0), (1, b_q, half))[0]
            low = lax.dynamic_slice(w_out_loc, (0, attn_cols + which * b_ff, 0), (1, b_ff, half))[0]
            return jnp.concatenate([top, low], axis=0)

        out_oth = across(out_rows(theirs))

        a_chunk = 1024
        q1_oth = across(w_in_loc[1, :, :attn_cols])
        in1_oth = []
        for c in range(ff // a_chunk):
            start = attn_cols + c * a_chunk
            in1_oth.append(across(jnp.concatenate([w_in_loc[1, :, start:start + a_chunk], w_in_loc[1, :, ff + start:ff + start + a_chunk]], axis=1)))
        o_chunk = 256
        out1_oth = [across(w_out_loc[1, :, c:c + o_chunk]) for c in range(0, half, o_chunk)]

        shift = (mine * (b_ff // 512)).astype(jnp.int32).reshape(1)
        none = jnp.zeros((1,), jnp.int32)

        w_qkv = jnp.concatenate([jnp.concatenate([cols(0, mine * b_q, b_q), q_oth], axis=0), w_kv[0]], axis=1)
        w_out0 = jnp.concatenate([out_rows(mine), out_oth], axis=1)
        groups = []
        for group, tokens in enumerate((normed, normed_oth)):
            h_full = gather_seq(tokens).reshape(rows, d_model)
            qkv = jnp.dot(h_full, w_qkv, preferred_element_type=F32).astype(BF16).reshape(n_batch, seq, -1)
            attn = attend(qkv, lens_all[group * n_batch:(group + 1) * n_batch], n_heads // 2, head_dim)
            lhs = [attn.reshape(rows, -1)]
            for c in range(b_ff // b_chunk):
                lhs.append(gated(h_full, w_in_loc, in_oth[c], 0, shift, attn_cols + c * b_chunk, attn_cols + ff + c * b_chunk, b_chunk))
            groups.append(lhs)
        z_parts = []
        for lhs in groups:
            z = project(lhs, w_out0).reshape(n_batch, seq, d_model)
            z_parts.append(scatter_seq(z))
        z_got = across(swap_halves(z_parts[1]))
        hidden = (hidden.astype(F32) + (z_parts[0].astype(F32) + z_got.astype(F32))).astype(BF16)

        gain1 = same(gamma[1:2])[0]
        normed = rms_norm(hidden, gain1)
        h_full = gather_seq(normed).reshape(rows, d_model)
        w_qkv = jnp.concatenate([jnp.concatenate([w_in_loc[1, :, :attn_cols], q1_oth], axis=0), w_kv[1]], axis=1)
        qkv = jnp.dot(h_full, w_qkv, preferred_element_type=F32).astype(BF16).reshape(n_batch, seq, -1)
        attn = attend(qkv, lens_loc, n_heads, head_dim)
        lhs = [attn.reshape(rows, -1)]
        for c in range(ff // a_chunk):
            lhs.append(gated(h_full, w_in_loc, in1_oth[c], 1, none, attn_cols + c * a_chunk, attn_cols + ff + c * a_chunk, a_chunk))
        z_all = [scatter_seq(project(lhs, w_out_loc, layer=1).reshape(n_batch, seq, half))]
        for piece in out1_oth:
            z_all.append(scatter_seq(project(lhs, piece).reshape(n_batch, seq, o_chunk)))
        z = jnp.concatenate(z_all, axis=-1)
        hidden = (hidden.astype(F32) + z.astype(F32)).astype(BF16)
        return own_first(hidden)

    in_specs = (
        P(batch_axes, "model", None),
        P(batch_axes),
        P(None, "data"),
        P(None, "data", "model"),
        P(None, "data", None),
        P(None, "model", "data"),
    )
    return jax.shard_map(local_body, mesh=mesh, in_specs=in_specs, out_specs=P(batch_axes, "model", None), check_vma=False)
```

```python
import functools

import jax
import jax.numpy as jnp
from jax import lax
from jax.experimental import pallas as pl
from jax.experimental.pallas import tpu as pltpu
from jax.sharding import PartitionSpec as P

EPSILON = 1e-6
PARAMS = pltpu.CompilerParams(vmem_limit_bytes=60 * 1024 * 1024)
BF16 = jnp.bfloat16
F32 = jnp.float32


def normalize(parts, gains):
    d_model = sum(p.shape[-1] for p in parts)
    square = sum(jnp.sum(p * p, axis=-1, keepdims=True) for p in parts)
    inv_rms = lax.rsqrt(square / d_model + EPSILON)
    return [(p * inv_rms * g.astype(F32)).astype(BF16) for p, g in zip(parts, gains)]


def first_norm_kernel(mine_ref, x_ref, gain_ref, hidden_ref, normed_ref):
    half = hidden_ref.shape[2]
    low, high = x_ref[:, :half], x_ref[:, half:]
    first = mine_ref[0] == 0
    parts = [jnp.where(first, low, high), jnp.where(first, high, low)]
    normed = normalize([p.astype(F32) for p in parts], [gain_ref[0:1, :], gain_ref[1:2, :]])
    for k in range(2):
        hidden_ref[k] = parts[k]
        normed_ref[k] = normed[k]


def first_norm(mine, x_loc, gain, which):
    _, seq_loc, d_model = x_loc.shape
    shape = (2, seq_loc, d_model // 2)
    whole = pl.BlockSpec(shape, lambda i, s: (0, 0, 0))
    return pl.pallas_call(
        first_norm_kernel,
        grid_spec=pltpu.PrefetchScalarGridSpec(
            num_scalar_prefetch=1,
            grid=(1,),
            in_specs=[pl.BlockSpec((None, seq_loc, d_model), lambda i, s: (which, 0, 0)), pl.BlockSpec(gain.shape, lambda i, s: (0, 0))],
            out_specs=[whole, whole],
        ),
        out_shape=[jax.ShapeDtypeStruct(shape, BF16)] * 2,
        compiler_params=PARAMS,
        cost_estimate=pl.CostEstimate(flops=3000000, bytes_accessed=6 * seq_loc * d_model, transcendentals=0),
        name="first_norm",
    )(mine, x_loc, gain)


def add_norm_kernel(hidden_ref, here_ref, there_ref, gain_ref, out_ref, normed_ref):
    parts = []
    for k in range(2):
        z = here_ref[k].astype(F32) + there_ref[1 - k].astype(F32)
        parts.append((hidden_ref[k].astype(F32) + z).astype(BF16))
        out_ref[k] = parts[k]
    normed = normalize([p.astype(F32) for p in parts], [gain_ref[0:1, :], gain_ref[1:2, :]])
    for k in range(2):
        normed_ref[k] = normed[k]


def add_norm(hidden, here, there, gain):
    return pl.pallas_call(
        add_norm_kernel,
        out_shape=[jax.ShapeDtypeStruct(hidden.shape, BF16)] * 2,
        compiler_params=PARAMS,
        cost_estimate=pl.CostEstimate(flops=4000000, bytes_accessed=10 * hidden.size, transcendentals=0),
        name="add_norm",
    )(hidden, here, there, gain)


def finish_kernel(mine_ref, *refs):
    *ins, out_ref = refs
    half = out_ref.shape[2] // 2
    first = mine_ref[0] == 0
    for c in range(out_ref.shape[0]):
        hidden_ref, own_ref, oth_ref = ins[3 * c:3 * c + 3]
        own = (hidden_ref[0].astype(F32) + own_ref[...].astype(F32)).astype(BF16)
        oth = (hidden_ref[1].astype(F32) + oth_ref[...].astype(F32)).astype(BF16)
        out_ref[c, :, :half] = jnp.where(first, own, oth)
        out_ref[c, :, half:] = jnp.where(first, oth, own)


def finish(mine, ins, shape):
    return pl.pallas_call(
        finish_kernel,
        in_specs=[pl.BlockSpec(memory_space=pltpu.SMEM)] + [pl.BlockSpec(memory_space=pltpu.VMEM)] * len(ins),
        out_shape=jax.ShapeDtypeStruct(shape, BF16),
        compiler_params=PARAMS,
        name="finish",
    )(mine, *ins)


def qkv_kernel(flip, idx_ref, h_ref, q_own, q_oth, kv_own, kv_oth, q_ref, kv_ref):
    h_a, h_b = (h_ref[1], h_ref[0]) if flip else (h_ref[0], h_ref[1])
    for own, oth, out in ((q_own, q_oth, q_ref), (kv_own, kv_oth, kv_ref)):
        total = jnp.dot(h_a, own[...], preferred_element_type=F32) + jnp.dot(h_b, oth[...], preferred_element_type=F32)
        out[...] = total.astype(BF16)


def qkv(h, flip, w_in, q_oth, w_kv, kv_oth, layer, idx, tile_m=512):
    _, rows, half = h.shape
    n_q, n_kv = q_oth.shape[1], w_kv.shape[2]
    return pl.pallas_call(
        functools.partial(qkv_kernel, flip),
        grid_spec=pltpu.PrefetchScalarGridSpec(
            num_scalar_prefetch=1,
            grid=(rows // tile_m,),
            in_specs=[
                pl.BlockSpec((2, tile_m, half), lambda m, s: (0, m, 0)),
                pl.BlockSpec((None, half, n_q), lambda m, s: (layer, 0, s[0])),
                pl.BlockSpec((half, n_q), lambda m, s: (0, 0)),
                pl.BlockSpec((None, half, n_kv), lambda m, s: (layer, 0, 0)),
                pl.BlockSpec((None, half, n_kv), lambda m, s: (layer, 0, 0)),
            ],
            out_specs=[pl.BlockSpec((tile_m, n_q), lambda m, s: (m, 0)), pl.BlockSpec((tile_m, n_kv), lambda m, s: (m, 0))],
        ),
        out_shape=[jax.ShapeDtypeStruct((rows, n_q), BF16), jax.ShapeDtypeStruct((rows, n_kv), BF16)],
        compiler_params=PARAMS,
        cost_estimate=pl.CostEstimate(flops=4 * rows * half * (n_q + n_kv), bytes_accessed=4 * rows * half + 4 * half * (n_q + n_kv), transcendentals=0),
        name="qkv",
    )(idx, h, w_in, q_oth, w_kv, kv_oth)


def gated_kernel(flip, idx_ref, h_ref, g_own, u_own, g_oth, u_oth, out_ref):
    h_a, h_b = (h_ref[1], h_ref[0]) if flip else (h_ref[0], h_ref[1])
    gate = jnp.dot(h_a, g_own[...], preferred_element_type=F32) + jnp.dot(h_b, g_oth[...], preferred_element_type=F32)
    up = jnp.dot(h_a, u_own[...], preferred_element_type=F32) + jnp.dot(h_b, u_oth[...], preferred_element_type=F32)
    gate = gate.astype(BF16).astype(F32)
    up = up.astype(BF16).astype(F32)
    out_ref[...] = (gate * jax.nn.sigmoid(gate) * up).astype(BF16)


def gated(h, flip, w_in, g_oth, u_oth, layer, idx, g_col, u_col, tile_m=1024, tile_n=512):
    _, rows, half = h.shape
    width = g_oth.shape[1]
    n_tiles = width // tile_n
    g_blk, u_blk = g_col // tile_n, u_col // tile_n
    return pl.pallas_call(
        functools.partial(gated_kernel, flip),
        grid_spec=pltpu.PrefetchScalarGridSpec(
            num_scalar_prefetch=1,
            grid=(n_tiles, rows // tile_m),
            in_specs=[
                pl.BlockSpec((2, tile_m, half), lambda n, m, s: (0, m, 0)),
                pl.BlockSpec((None, half, tile_n), lambda n, m, s: (layer, 0, g_blk + s[0] + n)),
                pl.BlockSpec((None, half, tile_n), lambda n, m, s: (layer, 0, u_blk + s[0] + n)),
                pl.BlockSpec((half, tile_n), lambda n, m, s: (0, n)),
                pl.BlockSpec((half, tile_n), lambda n, m, s: (0, n)),
            ],
            out_specs=pl.BlockSpec((tile_m, tile_n), lambda n, m, s: (m, n)),
        ),
        out_shape=jax.ShapeDtypeStruct((rows, width), BF16),
        compiler_params=PARAMS,
        cost_estimate=pl.CostEstimate(flops=8 * rows * half * width, bytes_accessed=4 * rows * half * n_tiles + 8 * half * width + 2 * rows * width, transcendentals=rows * width),
        name="gated",
    )(idx, h, w_in, w_in, g_oth, u_oth)


def project_kernel(n_lhs, set_sizes, *refs):
    lhs, out_ref = refs[:n_lhs], refs[-1]
    start = n_lhs
    for k, size in enumerate(set_sizes):
        weights = refs[start:start + size]
        start += size
        pos, row, acc = 0, 0, None
        for ref in lhs:
            depth = ref.shape[1]
            if row == weights[pos].shape[0]:
                pos, row = pos + 1, 0
            part = jnp.dot(ref[...], weights[pos][row:row + depth, :], preferred_element_type=F32)
            acc = part if acc is None else acc + part
            row += depth
        out_ref[k] = acc.astype(BF16)


def project(lhs, sets, layer=None, tile_m=1024, tile_n=512):
    rows = lhs[0].shape[0]
    depth = sum(a.shape[1] for a in lhs)
    cols = sets[0][0].shape[-1]
    specs = []
    for weights in sets:
        for w in weights:
            if layer is None:
                specs.append(pl.BlockSpec((w.shape[0], tile_n), lambda n, m: (0, n)))
            else:
                specs.append(pl.BlockSpec((None, w.shape[1], tile_n), lambda n, m: (layer, 0, n)))
    return pl.pallas_call(
        functools.partial(project_kernel, len(lhs), [len(weights) for weights in sets]),
        grid=(cols // tile_n, rows // tile_m),
        in_specs=[pl.BlockSpec((tile_m, a.shape[1]), lambda n, m: (m, 0)) for a in lhs] + specs,
        out_specs=pl.BlockSpec((len(sets), tile_m, tile_n), lambda n, m: (0, m, n)),
        out_shape=jax.ShapeDtypeStruct((len(sets), rows, cols), BF16),
        compiler_params=PARAMS,
        cost_estimate=pl.CostEstimate(flops=2 * rows * depth * cols * len(sets), bytes_accessed=2 * (rows * depth * (cols // tile_n) + depth * cols * len(sets) + rows * cols * len(sets)), transcendentals=0),
        name="project",
    )(*lhs, *[w for weights in sets for w in weights])


def attend_kernel(block, n_blocks, which_seq, lens_ref, q_ref, k_ref, v_ref, out_ref):
    seq_len = lens_ref[which_seq]
    which = pl.program_id(1)
    head_dim = q_ref.shape[1]
    for blk in range(n_blocks):
        @pl.when(which == blk)
        def _(blk=blk):
            keys = (blk + 1) * block
            scores = lax.dot_general(q_ref[...], k_ref[:keys, :], (((1,), (1,)), ((), ())), preferred_element_type=F32) * (head_dim ** -0.5)
            key_pos = lax.broadcasted_iota(jnp.int32, (block, keys), 1)
            q_pos = blk * block + lax.broadcasted_iota(jnp.int32, (block, keys), 0)
            scores = jnp.where((key_pos <= q_pos) & (key_pos < seq_len), scores, -1e30)
            top = jnp.max(scores, axis=-1, keepdims=True)
            weights = jnp.exp(scores - top)
            probs = (weights / jnp.sum(weights, axis=-1, keepdims=True)).astype(BF16)
            out_ref[...] = jnp.dot(probs, v_ref[:keys, :], preferred_element_type=F32).astype(BF16)


def attend(q, kv, lens, which_seq, block=512):
    length, width = q.shape
    head_dim = kv.shape[1] // 2
    n_heads, n_blocks = width // head_dim, length // block
    return pl.pallas_call(
        functools.partial(attend_kernel, block, n_blocks, which_seq),
        grid_spec=pltpu.PrefetchScalarGridSpec(
            num_scalar_prefetch=1,
            grid=(n_heads, n_blocks),
            in_specs=[
                pl.BlockSpec((block, head_dim), lambda i, b, s: (b, i)),
                pl.BlockSpec((length, head_dim), lambda i, b, s: (0, 0)),
                pl.BlockSpec((length, head_dim), lambda i, b, s: (0, 1)),
            ],
            out_specs=pl.BlockSpec((block, head_dim), lambda i, b, s: (b, i)),
        ),
        out_shape=jax.ShapeDtypeStruct((length, width), BF16),
        compiler_params=PARAMS,
        cost_estimate=pl.CostEstimate(flops=4 * n_heads * length * length * head_dim * 5 // 8, bytes_accessed=8 * length * width, transcendentals=n_heads * length * length),
        name="attend",
    )(lens, q, kv, kv)


def solution(mesh):
    batch_axes = ("rep", "data")
    n_model = mesh.shape["model"]
    swap = [(0, 1), (1, 0)]
    in0 = (1024, 1024)
    in1 = (1024, 512, 512, 1024, 1024)

    def across(value):
        return lax.ppermute(value, "data", swap)

    def gather(value):
        return lax.all_gather(value, "model", axis=1, tiled=True)

    def scatter(value):
        return lax.psum_scatter(value, "model", scatter_dimension=1, tiled=True)

    def local_body(x_loc, lens_loc, gamma_loc, w_in_loc, w_kv_loc, w_out_loc):
        half = gamma_loc.shape[1]
        kv_cols = w_kv_loc.shape[2]
        out_local = w_out_loc.shape[1]
        ff = w_in_loc.shape[2] - out_local
        attn_cols = out_local - ff
        b_q, b_ff = attn_cols // 2, ff // 2
        mine = lax.axis_index("data")
        theirs = 1 - mine
        slot = lax.axis_index("model")
        mine_arr = mine.astype(jnp.int32).reshape(1)
        shift = mine_arr * (b_ff // 512)
        none = jnp.zeros((1,), jnp.int32)

        def cols(start, width):
            return lax.dynamic_slice(w_in_loc, (0, 0, start), (1, half, width))[0]

        def out_rows(which):
            return [
                lax.dynamic_slice(w_out_loc, (0, which * b_q, 0), (1, b_q, half))[0],
                lax.dynamic_slice(w_out_loc, (0, attn_cols + which * b_ff, 0), (1, b_ff, half))[0],
            ]

        def gain(layer):
            return jnp.stack([gamma_loc[layer], gamma_oth[layer]])

        gamma_oth = across(gamma_loc)
        lens_oth = across(lens_loc)
        part = half // n_model
        kv_oth = gather(across(lax.dynamic_slice(w_kv_loc, (0, slot * part, 0), (2, part, kv_cols))))

        q0_oth = across(cols(theirs * b_q, b_q))
        in0_oth = []
        at = attn_cols + theirs * b_ff
        for width in in0:
            in0_oth.append((across(cols(at, width)), across(cols(ff + at, width))))
            at += width
        hidden, normed = [], []
        for c in range(2):
            x_c, n_c = first_norm(mine_arr, x_loc, gain(0), c)
            hidden.append(x_c)
            normed.append(n_c)
        h0_oth = [across(normed[c]) for c in range(2)]
        top, low = out_rows(theirs)
        out0_oth = [across(top), across(low)]
        q1_oth = across(w_in_loc[1, :, :attn_cols])
        in1_oth = []
        at = attn_cols
        for width in in1:
            in1_oth.append((across(w_in_loc[1, :, at:at + width]), across(w_in_loc[1, :, ff + at:ff + at + width])))
            at += width
        out1_oth = across(w_out_loc[1])

        lhs0 = {}
        for name, flip, tokens, lens, which in (("o0", False, normed[0], lens_loc, 0), ("o1", False, normed[1], lens_loc, 1), ("p0", True, h0_oth[0], lens_oth, 0), ("p1", True, h0_oth[1], lens_oth, 1)):
            h = gather(tokens)
            q, kv = qkv(h, flip, w_in_loc, q0_oth, w_kv_loc, kv_oth, 0, mine_arr)
            lhs = [attend(q, kv, lens, which)]
            at = attn_cols
            for c, width in enumerate(in0):
                lhs.append(gated(h, flip, w_in_loc, *in0_oth[c], 0, shift, at, ff + at))
                at += width
            lhs0[name] = lhs
        own_sets = out_rows(mine)
        z0 = {}
        for name, lhs in lhs0.items():
            z = project(lhs, [own_sets, out0_oth])
            z0[name] = scatter(z)
        z_got = [across(z0[f"p{c}"]) for c in range(2)]

        ends = []
        for c in range(2):
            x_c, n_c = add_norm(hidden[c], z0[f"o{c}"], z_got[c], gain(1))
            h = gather(n_c)
            q, kv = qkv(h, False, w_in_loc, q1_oth, w_kv_loc, kv_oth, 1, none)
            lhs = [attend(q, kv, lens_loc, c)]
            at = attn_cols
            for k, width in enumerate(in1):
                lhs.append(gated(h, False, w_in_loc, *in1_oth[k], 1, none, at, ff + at))
                at += width
            z_own = project(lhs, [[w_out_loc]], layer=1)
            z_oth = project(lhs, [[out1_oth]])
            ends += [x_c, scatter(z_own)[0], scatter(z_oth)[0]]
        return finish(mine_arr, ends, x_loc.shape)

    in_specs = (
        P(batch_axes, "model", None),
        P(batch_axes),
        P(None, "data"),
        P(None, "data", "model"),
        P(None, "data", None),
        P(None, "model", "data"),
    )
    return jax.shard_map(local_body, mesh=mesh, in_specs=in_specs, out_specs=P(batch_axes, "model", None), check_vma=False)
```
